32 devices in a mesh: row: 8 (over y, x, core), col: 4 (over z).
Axes of the slice: x: 2, y: 2, z: 4, core: 2. Of those that a mesh axis runs over, the one named last changes fastest.
Arguments:
- front_tiles: float32 [2, 2048, 2, 1024], P(None, 'row', None, 'col'), may hold values from -6 to 6, as said below
- lead_tiles: int32 [2, 8], P(None, 'row'), may hold values from 0 to 7
- damping: float32 [2, 1024], P(None, 'col'), may hold values from 1.5 to 6
Outputs:
- factor: float32 [2, 2048, 2, 1024], P(None, 'row', None, 'col')
The draws below stay inside these ranges and needn't reach their ends.
Inputs may be any that keep to these rules, and one draw needn't show every extreme that they name: `front_tiles`: the front's entries. `lead_tiles`: entries of the first 8 tile rows are not read.
All inputs are finite; a program needn't handle non-finite values.
Results may differ from the reference program's by a relative error of at most 0.00005.
Values sent between devices are 32-bit elements; how exact they have to be, the bound alone decides.
No kernel may reach another device: no remote copies, remote signals or barrier semaphores. Data moves between devices by JAX's collectives and lax.ppermute only.
A program may use at most 64 MiB of HBM per device.

```python
import math
import jax
import jax.numpy as jnp
from jax import lax

TILE = 256
COL_TILES = 8
RTD = 2
CTD = 2
N_ROW = 8
N_COL = 4


def draw_front_tiles(key, part):
    shape = (RTD, N_ROW * TILE, CTD, N_COL * TILE)
    row_shape = (RTD, N_ROW * TILE, 1, 1)
    values = jax.random.truncated_normal(key, -6.0, 6.0, shape, jnp.float32)
    row_scale = jnp.ones(row_shape, jnp.float32)
    slot_ids = lax.broadcasted_iota(jnp.int32, row_shape, 0)
    place_ids = lax.broadcasted_iota(jnp.int32, row_shape, 1)
    tile_row = slot_ids * N_ROW + place_ids // TILE
    scale = jnp.where(tile_row < COL_TILES, 0.5 / math.sqrt(COL_TILES * TILE), row_scale)
    return values * scale


def with_ends(values, rng, smallest, high):
    dims = values.shape
    place = [jax.random.randint(jax.random.fold_in(rng, axis), (), 0, dims[axis]) for axis in range(len(dims))]
    values = values.at[tuple(place)].set(smallest)
    longest = dims.index(max(dims))
    place[longest] = (place[longest] + 1) % dims[longest]
    return values.at[tuple(place)].set(high)


def block_scale(stream_key, shape, shards, least, high):
    loudness = 1.0
    for position, parts in shards:
        draws = jax.random.uniform(jax.random.fold_in(jax.random.fold_in(stream_key, 6), position), (parts,), jnp.float32, least / len(shards), high / len(shards))
        loudness = loudness * jnp.repeat(jnp.exp(draws), shape[position] // parts).reshape((-1,) + (1,) * (len(shape) - 1 - position))
    return loudness


def setup_inputs(seed: int = 0) -> dict:
    key_of = jax.random.split(jax.random.key(seed), 4)
    return {
        "front_tiles": draw_front_tiles(jax.random.fold_in(key_of[3], 71), 0),
        "lead_tiles": with_ends(jax.random.randint(key_of[1], (RTD, N_ROW), 0, COL_TILES), jax.random.fold_in(key_of[1], 1), 0, COL_TILES - 1).astype(jnp.int32),
        "damping": jnp.clip(jnp.exp(math.log(6.0) - 1.3862944 * jax.random.uniform(key_of[2], (CTD, N_COL * TILE), jnp.float32) ** block_scale(key_of[2], (CTD, N_COL * TILE), ((1, 4),), -0.2, 0.2)), 1.5, 6.0),
    }


def reference(front_tiles, lead_tiles, damping):
    row_total = RTD * N_ROW * TILE
    col_total = COL_TILES * TILE
    matrix = front_tiles.reshape(row_total, col_total)
    tile_ids = jnp.arange(RTD * N_ROW, dtype=jnp.int32)
    tile_lead = jnp.where(tile_ids < COL_TILES, 0, lead_tiles.reshape(-1).astype(jnp.int32))
    col_tile = jnp.arange(col_total, dtype=jnp.int32) // TILE
    kept_mask = col_tile[None, :] >= tile_lead[:, None]
    kept_rows = jnp.repeat(kept_mask, TILE, axis=0)
    matrix = jnp.where(kept_rows, matrix, jnp.zeros_like(matrix))
    separator = matrix[:col_total]
    tail_rows = matrix[col_total:]
    symmetric = jnp.tril(separator) + jnp.tril(separator, -1).T + jnp.diag(damping.reshape(-1))
    lower_factor = jnp.linalg.cholesky(symmetric)
    solved = jax.scipy.linalg.solve_triangular(lower_factor, tail_rows.T, lower=True).T
    stacked = jnp.concatenate([lower_factor, solved], axis=0)
    return stacked.reshape(front_tiles.shape)
```

```python
import jax
import jax.numpy as jnp
from jax import lax
from jax.sharding import PartitionSpec as P


def separator_tiles(sep_local, n_row, n_col, n_columns):
    sep_slots, tile, cslots, _ = sep_local.shape
    if sep_slots * n_row == n_columns:
        g = lax.all_gather(sep_local, ("row", "col"), axis=0)
        g = g.reshape(n_row, n_col, sep_slots, tile, cslots, tile)

        def get(i, j):
            return g[i % n_row, j % n_col, i // n_row, :, j // n_col, :]

        return get
    g = lax.all_gather(sep_local, "row", axis=1, tiled=True)
    g = g.reshape(sep_slots * n_row * tile, cslots, tile)[: n_columns * tile]
    g = lax.all_gather(g, "col", axis=2)

    def get(i, j):
        return g[i * tile:(i + 1) * tile, j // n_col, j % n_col, :]

    return get


def shards(front_tiles, lead_tiles, damping):
    slot_count, tile, col_slot_count, _ = front_tiles.shape
    n_row = lax.axis_size("row")
    n_col = lax.axis_size("col")
    row_at = lax.axis_index("row")
    col_at = lax.axis_index("col")
    n_columns = col_slot_count * n_col
    row_tiles = jnp.arange(slot_count, dtype=jnp.int32) * n_row + row_at
    col_tiles = jnp.arange(col_slot_count, dtype=jnp.int32) * n_col + col_at
    leads = jnp.where(row_tiles < n_columns, 0, lead_tiles[:, 0])
    kept_mask = col_tiles[None, :] >= leads[:, None]
    working = jnp.where(kept_mask[:, None, :, None], front_tiles, 0.0)

    sep_slots = -(-n_columns // n_row)
    get_tile = separator_tiles(working[:sep_slots], n_row, n_col, n_columns)
    damp_full = lax.all_gather(damping, "col", axis=1).reshape(n_columns, tile)

    tail_first = n_columns // n_row
    tail_slots = list(range(tail_first, slot_count))
    n_tail = len(tail_slots) * tile
    rows = lax.all_gather(working[tail_first:], "col", axis=3)
    rows = rows.reshape(n_tail, n_columns * tile)

    total_rows = n_columns * tile + n_tail
    factor = jnp.zeros((total_rows, n_columns * tile), jnp.float32)
    eye = jnp.eye(tile, dtype=jnp.float32)
    for k in range(n_columns):
        cols = slice(k * tile, (k + 1) * tile)
        diag = get_tile(k, k)
        diag = jnp.tril(diag) + jnp.tril(diag, -1).T + eye * damp_full[k][None, :]
        parts = [diag] + [get_tile(i, k) for i in range(k + 1, n_columns)] + [rows[:, cols]]
        panel = jnp.concatenate(parts, axis=0)
        if k > 0:
            left = factor[k * tile:, : k * tile]
            top = factor[k * tile:(k + 1) * tile, : k * tile]
            panel = panel - jnp.dot(left, top.T, precision=lax.Precision.HIGHEST,
                                    preferred_element_type=jnp.float32)
        lkk = jnp.tril(lax.linalg.cholesky(panel[:tile], symmetrize_input=True))
        below = lax.linalg.triangular_solve(lkk, panel[tile:], left_side=False, lower=True,
                                            transpose_a=True)
        factor = factor.at[k * tile:, cols].set(jnp.concatenate([lkk, below], axis=0))

    outs = []
    for slot in range(slot_count):
        tile_row = slot * n_row + row_at
        if slot < tail_first:
            start = tile_row * tile
        elif (slot + 1) * n_row <= n_columns:
            start = tile_row * tile
        else:
            tail_start = n_columns * tile + (slot - tail_first) * tile
            start = jnp.where(tile_row < n_columns, tile_row * tile, tail_start)
        picked = lax.dynamic_slice_in_dim(factor, start, tile, axis=0)
        picked = picked.reshape(tile, col_slot_count, n_col, tile)
        picked = lax.dynamic_index_in_dim(picked, col_at, axis=2, keepdims=False)
        outs.append(picked)
    return jnp.stack(outs, axis=0)


def solution(mesh):
    in_specs = (P(None, "row", None, "col"), P(None, "row"), P(None, "col"))
    out_specs = P(None, "row", None, "col")
    return jax.shard_map(shards, mesh=mesh, in_specs=in_specs, out_specs=out_specs, check_vma=False)
```

```python
import jax
import jax.numpy as jnp
from jax import lax
from jax.sharding import PartitionSpec as P

HIGHEST = lax.Precision.HIGHEST


def mm(a, b):
    return jnp.dot(a, b, precision=HIGHEST, preferred_element_type=jnp.float32)


def separator_tiles(sep_local, n_row, n_col, n_columns):
    sep_slots, tile, cslots, _ = sep_local.shape
    if sep_slots * n_row == n_columns:
        pieces = [lax.all_gather(sep_local[:, :, t, :], ("row", "col"), axis=0)
                  for t in range(cslots)]

        def get(i, j):
            g = pieces[j // n_col]
            return g[(i % n_row) * n_col + j % n_col, i // n_row]

        return get
    g = lax.all_gather(sep_local, "row", axis=1, tiled=True)
    g = g.reshape(sep_slots * n_row * tile, cslots, tile)[: n_columns * tile]
    g = lax.all_gather(g, "col", axis=2)

    def get(i, j):
        return g[i * tile:(i + 1) * tile, j // n_col, j % n_col, :]

    return get


def lower_inverse(lower):
    eye = jnp.eye(lower.shape[0], dtype=lower.dtype)
    return lax.linalg.triangular_solve(lower, eye, left_side=True, lower=True)


def factor_diag(diag):
    half = diag.shape[0] // 2
    l00 = jnp.tril(lax.linalg.cholesky(diag[:half, :half], symmetrize_input=False))
    i00 = lower_inverse(l00)
    l10 = mm(diag[half:, :half], i00.T)
    s11 = diag[half:, half:] - mm(l10, l10.T)
    l11 = jnp.tril(lax.linalg.cholesky(s11, symmetrize_input=True))
    i11 = lower_inverse(l11)
    i10 = -mm(i11, mm(l10, i00))
    zero = jnp.zeros((half, half), diag.dtype)
    lkk = jnp.block([[l00, zero], [l10, l11]])
    linv = jnp.block([[i00, zero], [i10, i11]])
    return lkk, linv


def shards(front_tiles, lead_tiles, damping):
    slot_count, tile, col_slot_count, _ = front_tiles.shape
    n_row = lax.axis_size("row")
    n_col = lax.axis_size("col")
    row_at = lax.axis_index("row")
    col_at = lax.axis_index("col")
    n_columns = col_slot_count * n_col
    row_tiles = jnp.arange(slot_count, dtype=jnp.int32) * n_row + row_at
    col_tiles = jnp.arange(col_slot_count, dtype=jnp.int32) * n_col + col_at
    leads = jnp.where(row_tiles < n_columns, 0, lead_tiles[:, 0])
    kept_mask = col_tiles[None, :] >= leads[:, None]
    working = jnp.where(kept_mask[:, None, :, None], front_tiles, 0.0)
    identity = jnp.eye(tile, dtype=jnp.float32)
    on_diagonal = (row_tiles[:, None] == col_tiles[None, :])[:, None, :, None]
    damp_term = identity[None, :, None, :] * damping[None, None, :, :]
    working = working + jnp.where(on_diagonal, damp_term, 0.0)

    sep_slots = -(-n_columns // n_row)
    get_tile = separator_tiles(working[:sep_slots], n_row, n_col, n_columns)

    tail_first = n_columns // n_row
    n_tail = (slot_count - tail_first) * tile
    tail_pieces = [lax.all_gather(working[tail_first:, :, t, :], "col", axis=2).reshape(n_tail, n_col * tile)
                   for t in range(col_slot_count)]

    total_rows = n_columns * tile + n_tail
    factor = jnp.zeros((total_rows, n_columns * tile), jnp.float32)
    for k in range(n_columns):
        cols = slice(k * tile, (k + 1) * tile)
        local = slice((k % n_col) * tile, (k % n_col + 1) * tile)
        parts = [get_tile(i, k) for i in range(k, n_columns)] + [tail_pieces[k // n_col][:, local]]
        panel = jnp.concatenate(parts, axis=0)
        if k > 0:
            left = factor[k * tile:, : k * tile]
            top = factor[k * tile:(k + 1) * tile, : k * tile]
            panel = panel - mm(left, top.T)
        diag = panel[:tile]
        diag = jnp.tril(diag) + jnp.tril(diag, -1).T
        lkk, linv = factor_diag(diag)
        below = mm(panel[tile:], linv.T)
        factor = factor.at[k * tile:, cols].set(jnp.concatenate([lkk, below], axis=0))

    outs = []
    for slot in range(slot_count):
        tile_row = slot * n_row + row_at
        if slot < tail_first:
            start = tile_row * tile
        else:
            tail_start = n_columns * tile + (slot - tail_first) * tile
            start = jnp.where(tile_row < n_columns, tile_row * tile, tail_start)
        picked = lax.dynamic_slice_in_dim(factor, start, tile, axis=0)
        picked = picked.reshape(tile, col_slot_count, n_col, tile)
        picked = lax.dynamic_index_in_dim(picked, col_at, axis=2, keepdims=False)
        outs.append(picked)
    return jnp.stack(outs, axis=0)


def solution(mesh):
    in_specs = (P(None, "row", None, "col"), P(None, "row"), P(None, "col"))
    out_specs = P(None, "row", None, "col")
    return jax.shard_map(shards, mesh=mesh, in_specs=in_specs, out_specs=out_specs, check_vma=False)
```

```python
import jax
import jax.numpy as jnp
from jax import lax
from jax.sharding import PartitionSpec as P

HIGHEST = lax.Precision.HIGHEST


def mm(a, b):
    return jnp.dot(a, b, precision=HIGHEST, preferred_element_type=jnp.float32)


def separator_tiles(sep_local, n_row, n_col, n_columns):
    sep_slots, tile, cslots, _ = sep_local.shape
    if sep_slots * n_row == n_columns:
        pieces = [lax.all_gather(sep_local[:, :, t, :], ("row", "col"), axis=0)
                  for t in range(cslots)]

        def get(i, j):
            g = pieces[j // n_col]
            return g[(i % n_row) * n_col + j % n_col, i // n_row]

        return get
    g = lax.all_gather(sep_local, "row", axis=1, tiled=True)
    g = g.reshape(sep_slots * n_row * tile, cslots, tile)[: n_columns * tile]
    g = lax.all_gather(g, "col", axis=2)

    def get(i, j):
        return g[i * tile:(i + 1) * tile, j // n_col, j % n_col, :]

    return get


def lower_inverse(lower):
    size = lower.shape[0]
    eye = jnp.eye(size, dtype=lower.dtype)
    diag = jnp.diagonal(lower)
    strict = jnp.tril(jnp.ones((size, size), jnp.bool_), -1)
    power = jnp.where(strict, -lower / diag[:, None], 0.0)
    product = eye + power
    span = 2
    while span < size:
        power = mm(power, power)
        product = mm(product, eye + power)
        span *= 2
    return product / diag[None, :]


def factor_diag(diag):
    half = diag.shape[0] // 2
    l00 = jnp.tril(lax.linalg.cholesky(diag[:half, :half], symmetrize_input=False))
    i00 = lower_inverse(l00)
    l10 = mm(diag[half:, :half], i00.T)
    s11 = diag[half:, half:] - mm(l10, l10.T)
    l11 = jnp.tril(lax.linalg.cholesky(s11, symmetrize_input=True))
    i11 = lower_inverse(l11)
    i10 = -mm(i11, mm(l10, i00))
    zero = jnp.zeros((half, half), diag.dtype)
    lkk = jnp.block([[l00, zero], [l10, l11]])
    linv = jnp.block([[i00, zero], [i10, i11]])
    return lkk, linv


def shards(front_tiles, lead_tiles, damping):
    slot_count, tile, col_slot_count, _ = front_tiles.shape
    n_row = lax.axis_size("row")
    n_col = lax.axis_size("col")
    row_at = lax.axis_index("row")
    col_at = lax.axis_index("col")
    n_columns = col_slot_count * n_col
    row_tiles = jnp.arange(slot_count, dtype=jnp.int32) * n_row + row_at
    col_tiles = jnp.arange(col_slot_count, dtype=jnp.int32) * n_col + col_at
    leads = jnp.where(row_tiles < n_columns, 0, lead_tiles[:, 0])
    kept_mask = col_tiles[None, :] >= leads[:, None]
    working = jnp.where(kept_mask[:, None, :, None], front_tiles, 0.0)
    identity = jnp.eye(tile, dtype=jnp.float32)
    on_diagonal = (row_tiles[:, None] == col_tiles[None, :])[:, None, :, None]
    damp_term = identity[None, :, None, :] * damping[None, None, :, :]
    working = working + jnp.where(on_diagonal, damp_term, 0.0)

    sep_slots = -(-n_columns // n_row)
    get_tile = separator_tiles(working[:sep_slots], n_row, n_col, n_columns)

    tail_first = n_columns // n_row
    n_tail = (slot_count - tail_first) * tile
    tail_pieces = [lax.all_gather(working[tail_first:, :, t, :], "col", axis=2).reshape(n_tail, n_col * tile)
                   for t in range(col_slot_count)]

    total_rows = n_columns * tile + n_tail
    factor = jnp.zeros((total_rows, n_columns * tile), jnp.float32)
    for k in range(n_columns):
        cols = slice(k * tile, (k + 1) * tile)
        local = slice((k % n_col) * tile, (k % n_col + 1) * tile)
        parts = [get_tile(i, k) for i in range(k, n_columns)] + [tail_pieces[k // n_col][:, local]]
        panel = jnp.concatenate(parts, axis=0)
        if k > 0:
            left = factor[k * tile:, : k * tile]
            top = factor[k * tile:(k + 1) * tile, : k * tile]
            panel = panel - mm(left, top.T)
        diag = panel[:tile]
        diag = jnp.tril(diag) + jnp.tril(diag, -1).T
        lkk, linv = factor_diag(diag)
        below = mm(panel[tile:], linv.T)
        factor = factor.at[k * tile:, cols].set(jnp.concatenate([lkk, below], axis=0))

    outs = []
    for slot in range(slot_count):
        tile_row = slot * n_row + row_at
        if slot < tail_first:
            start = tile_row * tile
        else:
            tail_start = n_columns * tile + (slot - tail_first) * tile
            start = jnp.where(tile_row < n_columns, tile_row * tile, tail_start)
        picked = lax.dynamic_slice_in_dim(factor, start, tile, axis=0)
        picked = picked.reshape(tile, col_slot_count, n_col, tile)
        picked = lax.dynamic_index_in_dim(picked, col_at, axis=2, keepdims=False)
        outs.append(picked)
    return jnp.stack(outs, axis=0)


def solution(mesh):
    in_specs = (P(None, "row", None, "col"), P(None, "row"), P(None, "col"))
    out_specs = P(None, "row", None, "col")
    return jax.shard_map(shards, mesh=mesh, in_specs=in_specs, out_specs=out_specs, check_vma=False)
```

```python
import jax
import jax.numpy as jnp
from jax import lax
from jax.sharding import PartitionSpec as P

HIGHEST = lax.Precision.HIGHEST


def mm(a, b):
    return jnp.dot(a, b, precision=HIGHEST, preferred_element_type=jnp.float32)


def separator_tiles(sep_local, n_row, n_col, n_columns, after_first):
    sep_slots, tile, cslots, _ = sep_local.shape
    if sep_slots * n_row == n_columns:
        pieces = []
        for t in range(cslots):
            piece = sep_local[:, :, t, :].reshape(sep_slots * tile, tile)
            if t == 1:
                piece, _ = lax.optimization_barrier((piece, after_first(pieces[0])))
            pieces.append(lax.all_gather(piece, ("row", "col"), axis=0))
        if cslots == 1:
            after_first(pieces[0])

        def get(i, j):
            g = pieces[j // n_col]
            row = (i // n_row) * tile
            return g[(i % n_row) * n_col + j % n_col, row:row + tile]

        return get
    after_first(None)
    g = lax.all_gather(sep_local, "row", axis=1, tiled=True)
    g = g.reshape(sep_slots * n_row * tile, cslots, tile)[: n_columns * tile]
    g = lax.all_gather(g, "col", axis=2)

    def get(i, j):
        return g[i * tile:(i + 1) * tile, j // n_col, j % n_col, :]

    return get


def lower_inverse(lower):
    size = lower.shape[0]
    eye = jnp.eye(size, dtype=lower.dtype)
    diag = jnp.sum(lower * eye, axis=1)
    strict = jnp.tril(jnp.ones((size, size), jnp.bool_), -1)
    power = jnp.where(strict, -lower / diag[:, None], 0.0)
    product = eye + power
    span = 2
    while span < size:
        power = mm(power, power)
        product = mm(product, eye + power)
        span *= 2
    return product / diag[None, :]


def factor_diag(diag):
    half = diag.shape[0] // 2
    l00 = jnp.tril(lax.linalg.cholesky(diag[:half, :half], symmetrize_input=False))
    i00 = lower_inverse(l00)
    l10 = mm(diag[half:, :half], i00.T)
    s11 = diag[half:, half:] - mm(l10, l10.T)
    l11 = jnp.tril(lax.linalg.cholesky(s11, symmetrize_input=True))
    i11 = lower_inverse(l11)
    i10 = -mm(i11, mm(l10, i00))
    zero = jnp.zeros((half, half), diag.dtype)
    lkk = jnp.block([[l00, zero], [l10, l11]])
    linv = jnp.block([[i00, zero], [i10, i11]])
    return lkk, linv


def shards(front_tiles, lead_tiles, damping):
    slot_count, tile, col_slot_count, _ = front_tiles.shape
    n_row = lax.axis_size("row")
    n_col = lax.axis_size("col")
    row_at = lax.axis_index("row")
    col_at = lax.axis_index("col")
    n_columns = col_slot_count * n_col
    row_tiles = jnp.arange(slot_count, dtype=jnp.int32) * n_row + row_at
    col_tiles = jnp.arange(col_slot_count, dtype=jnp.int32) * n_col + col_at
    leads = jnp.where(row_tiles < n_columns, 0, lead_tiles[:, 0])
    kept_mask = col_tiles[None, :] >= leads[:, None]
    working = jnp.where(kept_mask[:, None, :, None], front_tiles, 0.0)
    identity = jnp.eye(tile, dtype=jnp.float32)
    on_diagonal = (row_tiles[:, None] == col_tiles[None, :])[:, None, :, None]
    damp_term = identity[None, :, None, :] * damping[None, None, :, :]
    working = working + jnp.where(on_diagonal, damp_term, 0.0)

    tail_first = n_columns // n_row
    n_tail = (slot_count - tail_first) * tile
    tail_pieces = []

    def gather_tail(first_piece):
        tail_local = working[tail_first:]
        if first_piece is not None:
            tail_local, _ = lax.optimization_barrier((tail_local, first_piece))
        for t in range(col_slot_count):
            piece = tail_local[:, :, t, :].reshape(n_tail, tile)
            tail_pieces.append(lax.all_gather(piece, "col", axis=0))
        return tail_pieces[-1]

    sep_slots = -(-n_columns // n_row)
    get_tile = separator_tiles(working[:sep_slots], n_row, n_col, n_columns, gather_tail)

    sep_panels = []
    tail_panels = []
    for k in range(n_columns):
        parts = [get_tile(i, k) for i in range(k, n_columns)]
        panel = jnp.concatenate(parts, axis=0) if len(parts) > 1 else parts[0]
        tail_panel = tail_pieces[k // n_col][k % n_col]
        for m in range(k):
            rows = sep_panels[m][(k - m) * tile:]
            top = rows[:tile]
            panel = panel - mm(rows, top.T)
            tail_panel = tail_panel - mm(tail_panels[m], top.T)
        diag = panel[:tile]
        diag = jnp.tril(diag) + jnp.tril(diag, -1).T
        lkk, linv = factor_diag(diag)
        if k + 1 < n_columns:
            below = mm(panel[tile:], linv.T)
            sep_panels.append(jnp.concatenate([lkk, below], axis=0))
        else:
            sep_panels.append(lkk)
        tail_panels.append(mm(tail_panel, linv.T))

    outs = []
    for slot in range(slot_count):
        tile_row = slot * n_row + row_at
        blocks = []
        for t in range(col_slot_count):
            want = t * n_col + col_at
            sep_block = jnp.zeros((tile, tile), jnp.float32)
            tail_block = jnp.zeros((tile, tile), jnp.float32)
            for m in range(t * n_col, (t + 1) * n_col):
                offset = jnp.clip(tile_row - m, 0, n_columns - 1 - m) * tile
                candidate = lax.dynamic_slice_in_dim(sep_panels[m], offset, tile, axis=0)
                candidate = jnp.where(tile_row >= m, candidate, 0.0)
                sep_block = jnp.where(want == m, candidate, sep_block)
                if slot >= tail_first:
                    tail_rows = tail_panels[m][(slot - tail_first) * tile:(slot - tail_first + 1) * tile]
                    tail_block = jnp.where(want == m, tail_rows, tail_block)
            if slot >= tail_first:
                sep_block = jnp.where(tile_row < n_columns, sep_block, tail_block)
            blocks.append(sep_block)
        outs.append(jnp.stack(blocks, axis=1))
    return jnp.stack(outs, axis=0)


def solution(mesh):
    in_specs = (P(None, "row", None, "col"), P(None, "row"), P(None, "col"))
    out_specs = P(None, "row", None, "col")
    return jax.shard_map(shards, mesh=mesh, in_specs=in_specs, out_specs=out_specs, check_vma=False)
```

```python
import jax
import jax.numpy as jnp
from jax import lax
from jax.sharding import PartitionSpec as P

HIGHEST = lax.Precision.HIGHEST


def mm(a, b):
    return jnp.dot(a, b, precision=HIGHEST, preferred_element_type=jnp.float32)


def separator_tiles(sep_local, n_row, n_col, n_columns, after_first):
    sep_slots, tile, cslots, _ = sep_local.shape
    if sep_slots * n_row == n_columns:
        pieces = []
        for t in range(cslots):
            piece = sep_local[:, :, t, :].reshape(sep_slots * tile, tile)
            if t == 1:
                piece, _ = lax.optimization_barrier((piece, after_first(pieces[0])))
            pieces.append(lax.all_gather(piece, ("row", "col"), axis=0))
        if cslots == 1:
            after_first(pieces[0])

        def get(i, j):
            g = pieces[j // n_col]
            row = (i // n_row) * tile
            return g[(i % n_row) * n_col + j % n_col, row:row + tile]

        return get
    after_first(None)
    g = lax.all_gather(sep_local, "row", axis=1, tiled=True)
    g = g.reshape(sep_slots * n_row * tile, cslots, tile)[: n_columns * tile]
    g = lax.all_gather(g, "col", axis=2)

    def get(i, j):
        return g[i * tile:(i + 1) * tile, j // n_col, j % n_col, :]

    return get


def lower_inverse(lower):
    size = lower.shape[0]
    eye = jnp.eye(size, dtype=lower.dtype)
    diag = jnp.sum(lower * eye, axis=1)
    strict = jnp.tril(jnp.ones((size, size), jnp.bool_), -1)
    power = jnp.where(strict, -lower / diag[:, None], 0.0)
    product = eye + power
    span = 2
    while span < size:
        power = mm(power, power)
        product = mm(product, eye + power)
        span *= 2
    return product / diag[None, :]


def factor_diag(diag):
    half = diag.shape[0] // 2
    l00 = jnp.tril(lax.linalg.cholesky(diag[:half, :half], symmetrize_input=False))
    i00 = lower_inverse(l00)
    l10 = mm(diag[half:, :half], i00.T)
    s11 = diag[half:, half:] - mm(l10, l10.T)
    l11 = jnp.tril(lax.linalg.cholesky(s11, symmetrize_input=True))
    i11 = lower_inverse(l11)
    i10 = -mm(i11, mm(l10, i00))
    zero = jnp.zeros((half, half), diag.dtype)
    lkk = jnp.block([[l00, zero], [l10, l11]])
    linv = jnp.block([[i00, zero], [i10, i11]])
    return lkk, linv


def shards(front_tiles, lead_tiles, damping):
    slot_count, tile, col_slot_count, _ = front_tiles.shape
    n_row = lax.axis_size("row")
    n_col = lax.axis_size("col")
    row_at = lax.axis_index("row")
    col_at = lax.axis_index("col")
    n_columns = col_slot_count * n_col
    row_tiles = jnp.arange(slot_count, dtype=jnp.int32) * n_row + row_at
    col_tiles = jnp.arange(col_slot_count, dtype=jnp.int32) * n_col + col_at
    leads = jnp.where(row_tiles < n_columns, 0, lead_tiles[:, 0])
    kept_mask = col_tiles[None, :] >= leads[:, None]
    working = jnp.where(kept_mask[:, None, :, None], front_tiles, 0.0)
    identity = jnp.eye(tile, dtype=jnp.float32)
    on_diagonal = (row_tiles[:, None] == col_tiles[None, :])[:, None, :, None]
    damp_term = identity[None, :, None, :] * damping[None, None, :, :]
    working = working + jnp.where(on_diagonal, damp_term, 0.0)

    tail_first = n_columns // n_row
    n_tail = (slot_count - tail_first) * tile
    tail_pieces = []

    def gather_tail(first_piece):
        tail_local = working[tail_first:]
        if first_piece is not None:
            tail_local, _ = lax.optimization_barrier((tail_local, first_piece))
        for t in range(col_slot_count):
            piece = tail_local[:, :, t, :].reshape(n_tail, tile)
            tail_pieces.append(lax.all_gather(piece, "col", axis=0))
        return tail_pieces[-1]

    sep_slots = -(-n_columns // n_row)
    get_tile = separator_tiles(working[:sep_slots], n_row, n_col, n_columns, gather_tail)

    total_rows = n_columns * tile + n_tail
    factor = jnp.zeros((total_rows, n_columns * tile), jnp.float32)
    for k in range(n_columns):
        cols = slice(k * tile, (k + 1) * tile)
        parts = [get_tile(i, k) for i in range(k, n_columns)] + [tail_pieces[k // n_col][k % n_col]]
        panel = jnp.concatenate(parts, axis=0)
        if k > 0:
            left = factor[k * tile:, : k * tile]
            top = factor[k * tile:(k + 1) * tile, : k * tile]
            panel = panel - mm(left, top.T)
        diag = panel[:tile]
        diag = jnp.tril(diag) + jnp.tril(diag, -1).T
        lkk, linv = factor_diag(diag)
        below = mm(panel[tile:], linv.T)
        factor = factor.at[k * tile:, cols].set(jnp.concatenate([lkk, below], axis=0))

    outs = []
    for slot in range(slot_count):
        tile_row = slot * n_row + row_at
        if slot < tail_first:
            start = tile_row * tile
        else:
            tail_start = n_columns * tile + (slot - tail_first) * tile
            start = jnp.where(tile_row < n_columns, tile_row * tile, tail_start)
        picked = lax.dynamic_slice_in_dim(factor, start, tile, axis=0)
        picked = picked.reshape(tile, col_slot_count, n_col, tile)
        picked = lax.dynamic_index_in_dim(picked, col_at, axis=2, keepdims=False)
        outs.append(picked)
    return jnp.stack(outs, axis=0)


def solution(mesh):
    in_specs = (P(None, "row", None, "col"), P(None, "row"), P(None, "col"))
    out_specs = P(None, "row", None, "col")
    return jax.shard_map(shards, mesh=mesh, in_specs=in_specs, out_specs=out_specs, check_vma=False)
```

```python
import jax
import jax.numpy as jnp
from jax import lax
from jax.sharding import PartitionSpec as P

HIGHEST = lax.Precision.HIGHEST


def mm(a, b):
    return jnp.dot(a, b, precision=HIGHEST, preferred_element_type=jnp.float32)


def separator_tiles(sep_local, n_row, n_col, n_columns, after_first):
    sep_slots, tile, cslots, _ = sep_local.shape
    if sep_slots * n_row == n_columns:
        pieces = []
        for t in range(cslots):
            piece = sep_local[:, :, t, :].reshape(sep_slots * tile, tile)
            if t == 1:
                piece = piece + after_first(pieces[0])
            pieces.append(lax.all_gather(piece, ("row", "col"), axis=0))
        if cslots == 1:
            after_first(pieces[0])

        def get(i, j):
            g = pieces[j // n_col]
            row = (i // n_row) * tile
            return g[(i % n_row) * n_col + j % n_col, row:row + tile]

        return get
    after_first(None)
    g = lax.all_gather(sep_local, "row", axis=1, tiled=True)
    g = g.reshape(sep_slots * n_row * tile, cslots, tile)[: n_columns * tile]
    g = lax.all_gather(g, "col", axis=2)

    def get(i, j):
        return g[i * tile:(i + 1) * tile, j // n_col, j % n_col, :]

    return get


def after(value):
    return value.reshape(-1)[0] * 0.0


def lower_inverse(lower):
    size = lower.shape[0]
    eye = jnp.eye(size, dtype=lower.dtype)
    diag = jnp.sum(lower * eye, axis=1)
    strict = jnp.tril(jnp.ones((size, size), jnp.bool_), -1)
    power = jnp.where(strict, -lower / diag[:, None], 0.0)
    product = eye + power
    span = 2
    while span < size:
        power = mm(power, power)
        product = mm(product, eye + power)
        span *= 2
    return product / diag[None, :]


def factor_diag(diag):
    half = diag.shape[0] // 2
    l00 = jnp.tril(lax.linalg.cholesky(diag[:half, :half], symmetrize_input=False))
    i00 = lower_inverse(l00)
    l10 = mm(diag[half:, :half], i00.T)
    s11 = diag[half:, half:] - mm(l10, l10.T)
    l11 = jnp.tril(lax.linalg.cholesky(s11, symmetrize_input=True))
    i11 = lower_inverse(l11)
    i10 = -mm(i11, mm(l10, i00))
    zero = jnp.zeros((half, half), diag.dtype)
    lkk = jnp.block([[l00, zero], [l10, l11]])
    linv = jnp.block([[i00, zero], [i10, i11]])
    return lkk, linv


def shards(front_tiles, lead_tiles, damping):
    slot_count, tile, col_slot_count, _ = front_tiles.shape
    n_row = lax.axis_size("row")
    n_col = lax.axis_size("col")
    row_at = lax.axis_index("row")
    col_at = lax.axis_index("col")
    n_columns = col_slot_count * n_col
    row_tiles = jnp.arange(slot_count, dtype=jnp.int32) * n_row + row_at
    col_tiles = jnp.arange(col_slot_count, dtype=jnp.int32) * n_col + col_at
    leads = jnp.where(row_tiles < n_columns, 0, lead_tiles[:, 0])
    kept_mask = col_tiles[None, :] >= leads[:, None]
    working = jnp.where(kept_mask[:, None, :, None], front_tiles, 0.0)
    identity = jnp.eye(tile, dtype=jnp.float32)
    on_diagonal = (row_tiles[:, None] == col_tiles[None, :])[:, None, :, None]
    damp_term = identity[None, :, None, :] * damping[None, None, :, :]
    working = working + jnp.where(on_diagonal, damp_term, 0.0)

    tail_first = n_columns // n_row
    n_tail = (slot_count - tail_first) * tile
    tail_pieces = []

    def gather_tail(first_piece):
        tail_local = working[tail_first:]
        if first_piece is not None:
            tail_local = tail_local + after(first_piece)
        for t in range(col_slot_count):
            piece = tail_local[:, :, t, :].reshape(n_tail, tile)
            tail_pieces.append(lax.all_gather(piece, "col", axis=0))
        return after(tail_pieces[-1])

    sep_slots = -(-n_columns // n_row)
    get_tile = separator_tiles(working[:sep_slots], n_row, n_col, n_columns, gather_tail)

    total_rows = n_columns * tile + n_tail
    factor = jnp.zeros((total_rows, n_columns * tile), jnp.float32)
    for k in range(n_columns):
        cols = slice(k * tile, (k + 1) * tile)
        parts = [get_tile(i, k) for i in range(k, n_columns)] + [tail_pieces[k // n_col][k % n_col]]
        panel = jnp.concatenate(parts, axis=0)
        if k > 0:
            left = factor[k * tile:, : k * tile]
            top = factor[k * tile:(k + 1) * tile, : k * tile]
            panel = panel - mm(left, top.T)
        diag = panel[:tile]
        diag = jnp.tril(diag) + jnp.tril(diag, -1).T
        lkk, linv = factor_diag(diag)
        below = mm(panel[tile:], linv.T)
        factor = factor.at[k * tile:, cols].set(jnp.concatenate([lkk, below], axis=0))

    outs = []
    for slot in range(slot_count):
        tile_row = slot * n_row + row_at
        if slot < tail_first:
            start = tile_row * tile
        else:
            tail_start = n_columns * tile + (slot - tail_first) * tile
            start = jnp.where(tile_row < n_columns, tile_row * tile, tail_start)
        picked = lax.dynamic_slice_in_dim(factor, start, tile, axis=0)
        picked = picked.reshape(tile, col_slot_count, n_col, tile)
        picked = lax.dynamic_index_in_dim(picked, col_at, axis=2, keepdims=False)
        outs.append(picked)
    return jnp.stack(outs, axis=0)


def solution(mesh):
    in_specs = (P(None, "row", None, "col"), P(None, "row"), P(None, "col"))
    out_specs = P(None, "row", None, "col")
    return jax.shard_map(shards, mesh=mesh, in_specs=in_specs, out_specs=out_specs, check_vma=False)
```

```python
import jax
import jax.numpy as jnp
from jax import lax
from jax.sharding import PartitionSpec as P

HIGHEST = lax.Precision.HIGHEST


def mm(a, b):
    return jnp.dot(a, b, precision=HIGHEST, preferred_element_type=jnp.float32)


def separator_panels(sep_local, n_row, n_col, n_columns, after_first):
    sep_slots, tile, cslots, _ = sep_local.shape
    if sep_slots == 1 and n_row == n_columns:
        pieces = []
        for t in range(cslots):
            piece = sep_local[0, :, t, :]
            if t == 1:
                piece = piece + after_first(pieces[0])
            pieces.append(lax.all_gather(piece, ("col", "row"), axis=0))
        if cslots == 1:
            after_first(pieces[0])

        def panel(k):
            base = (k % n_col) * n_row
            return pieces[k // n_col][base + k:base + n_row].reshape((n_columns - k) * tile, tile)

        return panel
    after_first(None)
    g = lax.all_gather(sep_local, "row", axis=1, tiled=True)
    g = g.reshape(sep_slots * n_row * tile, cslots, tile)[: n_columns * tile]
    g = lax.all_gather(g, "col", axis=2)

    def panel(k):
        return g[k * tile:, k // n_col, k % n_col, :]

    return panel


def after(value):
    return value.reshape(-1)[0] * 0.0


def lower_inverse(lower):
    size = lower.shape[0]
    eye = jnp.eye(size, dtype=lower.dtype)
    diag = jnp.sum(lower * eye, axis=1)
    strict = jnp.tril(jnp.ones((size, size), jnp.bool_), -1)
    power = jnp.where(strict, -lower / diag[:, None], 0.0)
    product = eye + power
    span = 2
    while span < size:
        power = mm(power, power)
        product = mm(product, eye + power)
        span *= 2
    return product / diag[None, :]


def factor_diag(diag):
    half = diag.shape[0] // 2
    l00 = jnp.tril(lax.linalg.cholesky(diag[:half, :half], symmetrize_input=False))
    i00 = lower_inverse(l00)
    l10 = mm(diag[half:, :half], i00.T)
    s11 = diag[half:, half:] - mm(l10, l10.T)
    l11 = jnp.tril(lax.linalg.cholesky(s11, symmetrize_input=True))
    i11 = lower_inverse(l11)
    i10 = -mm(i11, mm(l10, i00))
    zero = jnp.zeros((half, half), diag.dtype)
    lkk = jnp.block([[l00, zero], [l10, l11]])
    linv = jnp.block([[i00, zero], [i10, i11]])
    return lkk, linv


def shards(front_tiles, lead_tiles, damping):
    slot_count, tile, col_slot_count, _ = front_tiles.shape
    n_row = lax.axis_size("row")
    n_col = lax.axis_size("col")
    row_at = lax.axis_index("row")
    col_at = lax.axis_index("col")
    n_columns = col_slot_count * n_col
    row_tiles = jnp.arange(slot_count, dtype=jnp.int32) * n_row + row_at
    col_tiles = jnp.arange(col_slot_count, dtype=jnp.int32) * n_col + col_at
    leads = jnp.where(row_tiles < n_columns, 0, lead_tiles[:, 0])
    kept_mask = col_tiles[None, :] >= leads[:, None]
    working = jnp.where(kept_mask[:, None, :, None], front_tiles, 0.0)
    identity = jnp.eye(tile, dtype=jnp.float32)
    on_diagonal = (row_tiles[:, None] == col_tiles[None, :])[:, None, :, None]
    damp_term = identity[None, :, None, :] * damping[None, None, :, :]
    working = working + jnp.where(on_diagonal, damp_term, 0.0)

    tail_first = n_columns // n_row
    n_tail = (slot_count - tail_first) * tile
    tail_pieces = []

    def gather_tail(first_piece):
        tail_local = working[tail_first:]
        if first_piece is not None:
            tail_local = tail_local + after(first_piece)
        for t in range(col_slot_count):
            piece = tail_local[:, :, t, :].reshape(n_tail, tile)
            tail_pieces.append(lax.all_gather(piece, "col", axis=0))
        return after(tail_pieces[-1])

    sep_slots = -(-n_columns // n_row)
    get_panel = separator_panels(working[:sep_slots], n_row, n_col, n_columns, gather_tail)

    total_rows = n_columns * tile + n_tail
    factor = jnp.zeros((total_rows, n_columns * tile), jnp.float32)
    for k in range(n_columns):
        cols = slice(k * tile, (k + 1) * tile)
        panel = jnp.concatenate([get_panel(k), tail_pieces[k // n_col][k % n_col]], axis=0)
        if k > 0:
            left = factor[k * tile:, : k * tile]
            top = factor[k * tile:(k + 1) * tile, : k * tile]
            panel = panel - mm(left, top.T)
        diag = panel[:tile]
        diag = jnp.tril(diag) + jnp.tril(diag, -1).T
        lkk, linv = factor_diag(diag)
        below = mm(panel[tile:], linv.T)
        factor = factor.at[k * tile:, cols].set(jnp.concatenate([lkk, below], axis=0))

    outs = []
    for slot in range(slot_count):
        tile_row = slot * n_row + row_at
        if slot < tail_first:
            start = tile_row * tile
        else:
            tail_start = n_columns * tile + (slot - tail_first) * tile
            start = jnp.where(tile_row < n_columns, tile_row * tile, tail_start)
        picked = lax.dynamic_slice_in_dim(factor, start, tile, axis=0)
        picked = picked.reshape(tile, col_slot_count, n_col, tile)
        picked = lax.dynamic_index_in_dim(picked, col_at, axis=2, keepdims=False)
        outs.append(picked)
    return jnp.stack(outs, axis=0)


def solution(mesh):
    in_specs = (P(None, "row", None, "col"), P(None, "row"), P(None, "col"))
    out_specs = P(None, "row", None, "col")
    return jax.shard_map(shards, mesh=mesh, in_specs=in_specs, out_specs=out_specs, check_vma=False)
```

```python
import jax
import jax.numpy as jnp
from jax import lax
from jax.sharding import PartitionSpec as P

HIGHEST = lax.Precision.HIGHEST


def mm(a, b, precision=HIGHEST):
    return jnp.dot(a, b, precision=precision, preferred_element_type=jnp.float32)


def separator_panels(sep_local, n_row, n_col, n_columns, after_first):
    sep_slots, tile, cslots, _ = sep_local.shape
    if sep_slots == 1 and n_row == n_columns:
        pieces = []
        for t in range(cslots):
            piece = sep_local[0, :, t, :]
            if t == 1:
                piece = piece + after_first(pieces[0])
            pieces.append(lax.all_gather(piece, ("col", "row"), axis=0))
        if cslots == 1:
            after_first(pieces[0])

        def panel(k):
            base = (k % n_col) * n_row
            return pieces[k // n_col][base + k:base + n_row].reshape((n_columns - k) * tile, tile)

        return panel
    after_first(None)
    g = lax.all_gather(sep_local, "row", axis=1, tiled=True)
    g = g.reshape(sep_slots * n_row * tile, cslots, tile)[: n_columns * tile]
    g = lax.all_gather(g, "col", axis=2)

    def panel(k):
        return g[k * tile:, k // n_col, k % n_col, :]

    return panel


def after(value):
    return value.reshape(-1)[0] * 0.0


def lower_inverse(lower):
    size = lower.shape[0]
    eye = jnp.eye(size, dtype=lower.dtype)
    diag = jnp.sum(lower * eye, axis=1)
    strict = jnp.tril(jnp.ones((size, size), jnp.bool_), -1)
    power = jnp.where(strict, -lower / diag[:, None], 0.0)
    product = eye + power
    span = 2
    while span < size:
        power = mm(power, power)
        product = mm(product, eye + power)
        span *= 2
    return product / diag[None, :]


def factor_diag(diag):
    half = diag.shape[0] // 2
    l00 = jnp.tril(lax.linalg.cholesky(diag[:half, :half], symmetrize_input=False))
    i00 = lower_inverse(l00)
    l10 = mm(diag[half:, :half], i00.T)
    s11 = diag[half:, half:] - mm(l10, l10.T)
    l11 = jnp.tril(lax.linalg.cholesky(s11, symmetrize_input=True))
    i11 = lower_inverse(l11)
    i10 = -mm(i11, mm(l10, i00))
    zero = jnp.zeros((half, half), diag.dtype)
    lkk = jnp.block([[l00, zero], [l10, l11]])
    linv = jnp.block([[i00, zero], [i10, i11]])
    return lkk, linv


def shards(front_tiles, lead_tiles, damping):
    slot_count, tile, col_slot_count, _ = front_tiles.shape
    n_row = lax.axis_size("row")
    n_col = lax.axis_size("col")
    row_at = lax.axis_index("row")
    col_at = lax.axis_index("col")
    n_columns = col_slot_count * n_col
    row_tiles = jnp.arange(slot_count, dtype=jnp.int32) * n_row + row_at
    col_tiles = jnp.arange(col_slot_count, dtype=jnp.int32) * n_col + col_at
    leads = jnp.where(row_tiles < n_columns, 0, lead_tiles[:, 0])
    kept_mask = col_tiles[None, :] >= leads[:, None]
    working = jnp.where(kept_mask[:, None, :, None], front_tiles, 0.0)
    identity = jnp.eye(tile, dtype=jnp.float32)
    on_diagonal = (row_tiles[:, None] == col_tiles[None, :])[:, None, :, None]
    damp_term = identity[None, :, None, :] * damping[None, None, :, :]
    working = working + jnp.where(on_diagonal, damp_term, 0.0)

    tail_first = n_columns // n_row
    n_tail = (slot_count - tail_first) * tile
    tail_pieces = []
    tail_sources = []

    def gather_tail(first_piece):
        tail_local = working[tail_first:]
        if first_piece is not None:
            tail_local = tail_local + after(first_piece)
        tail_sources.append(tail_local)
        for t in range(col_slot_count):
            piece = tail_local[:, :, t, :].reshape(n_tail, tile)
            tail_pieces.append(lax.all_gather(piece, "col", axis=0))
        return after(tail_pieces[-1])

    sep_slots = -(-n_columns // n_row)
    get_panel = separator_panels(working[:sep_slots], n_row, n_col, n_columns, gather_tail)

    total_rows = n_columns * tile + n_tail
    factor = jnp.zeros((total_rows, n_columns * tile), jnp.float32)
    for k in range(n_columns):
        cols = slice(k * tile, (k + 1) * tile)
        panel = jnp.concatenate([get_panel(k), tail_pieces[k // n_col][k % n_col]], axis=0)
        if k > 0:
            left = factor[k * tile:, : k * tile]
            top = factor[k * tile:(k + 1) * tile, : k * tile]
            panel = panel - mm(left, top.T, lax.Precision.HIGH)
        diag = panel[:tile]
        if k == 0:
            diag = diag + after(tail_sources[0])
        diag = jnp.tril(diag) + jnp.tril(diag, -1).T
        lkk, linv = factor_diag(diag)
        below = mm(panel[tile:], linv.T)
        factor = factor.at[k * tile:, cols].set(jnp.concatenate([lkk, below], axis=0))

    outs = []
    for slot in range(slot_count):
        tile_row = slot * n_row + row_at
        if slot < tail_first:
            start = tile_row * tile
        else:
            tail_start = n_columns * tile + (slot - tail_first) * tile
            start = jnp.where(tile_row < n_columns, tile_row * tile, tail_start)
        picked = lax.dynamic_slice_in_dim(factor, start, tile, axis=0)
        picked = picked.reshape(tile, col_slot_count, n_col, tile)
        picked = lax.dynamic_index_in_dim(picked, col_at, axis=2, keepdims=False)
        outs.append(picked)
    return jnp.stack(outs, axis=0)


def solution(mesh):
    in_specs = (P(None, "row", None, "col"), P(None, "row"), P(None, "col"))
    out_specs = P(None, "row", None, "col")
    return jax.shard_map(shards, mesh=mesh, in_specs=in_specs, out_specs=out_specs, check_vma=False)
```

```python
import jax
import jax.numpy as jnp
from jax import lax
from jax.sharding import PartitionSpec as P

HIGHEST = lax.Precision.HIGHEST


def mm(a, b, precision=HIGHEST):
    return jnp.dot(a, b, precision=precision, preferred_element_type=jnp.float32)


def separator_panels(sep_local, n_row, n_col, n_columns, after_first):
    sep_slots, tile, cslots, _ = sep_local.shape
    if sep_slots == 1 and n_row == n_columns:
        pieces = []
        for t in range(cslots):
            piece = sep_local[0, :, t, :]
            if t == 1:
                piece = piece + after_first(pieces[0])
            pieces.append(lax.all_gather(piece, ("col", "row"), axis=0))
        if cslots == 1:
            after_first(pieces[0])

        def panel(k):
            base = (k % n_col) * n_row
            return pieces[k // n_col][base + k:base + n_row].reshape((n_columns - k) * tile, tile)

        return panel
    after_first(None)
    g = lax.all_gather(sep_local, "row", axis=1, tiled=True)
    g = g.reshape(sep_slots * n_row * tile, cslots, tile)[: n_columns * tile]
    g = lax.all_gather(g, "col", axis=2)

    def panel(k):
        return g[k * tile:, k // n_col, k % n_col, :]

    return panel


def after(value):
    return value.reshape(-1)[0] * 0.0


def lower_inverse(lower):
    size = lower.shape[0]
    eye = jnp.eye(size, dtype=lower.dtype)
    diag = jnp.sum(lower * eye, axis=1)
    strict = jnp.tril(jnp.ones((size, size), jnp.bool_), -1)
    power = jnp.where(strict, -lower / diag[:, None], 0.0)
    product = eye + power
    span = 2
    while span < size:
        power = mm(power, power)
        product = mm(product, eye + power)
        span *= 2
    return product / diag[None, :]


def factor_diag(diag):
    half = diag.shape[0] // 2
    l00 = jnp.tril(lax.linalg.cholesky(diag[:half, :half], symmetrize_input=False))
    i00 = lower_inverse(l00)
    l10 = mm(diag[half:, :half], i00.T)
    s11 = diag[half:, half:] - mm(l10, l10.T)
    l11 = jnp.tril(lax.linalg.cholesky(s11, symmetrize_input=True))
    i11 = lower_inverse(l11)
    i10 = -mm(i11, mm(l10, i00))
    zero = jnp.zeros((half, half), diag.dtype)
    lkk = jnp.block([[l00, zero], [l10, l11]])
    linv = jnp.block([[i00, zero], [i10, i11]])
    return lkk, linv


def shards(front_tiles, lead_tiles, damping):
    slot_count, tile, col_slot_count, _ = front_tiles.shape
    n_row = lax.axis_size("row")
    n_col = lax.axis_size("col")
    row_at = lax.axis_index("row")
    col_at = lax.axis_index("col")
    n_columns = col_slot_count * n_col
    row_tiles = jnp.arange(slot_count, dtype=jnp.int32) * n_row + row_at
    col_tiles = jnp.arange(col_slot_count, dtype=jnp.int32) * n_col + col_at
    leads = jnp.where(row_tiles < n_columns, 0, lead_tiles[:, 0])
    kept_mask = col_tiles[None, :] >= leads[:, None]
    working = jnp.where(kept_mask[:, None, :, None], front_tiles, 0.0)
    identity = jnp.eye(tile, dtype=jnp.float32)
    on_diagonal = (row_tiles[:, None] == col_tiles[None, :])[:, None, :, None]
    damp_term = identity[None, :, None, :] * damping[None, None, :, :]
    working = working + jnp.where(on_diagonal, damp_term, 0.0)

    tail_first = n_columns // n_row
    n_tail = (slot_count - tail_first) * tile
    tail_pieces = []

    def gather_tail(first_piece):
        tail_local = working[tail_first:]
        if first_piece is not None:
            tail_local = tail_local + after(first_piece)
        for t in range(col_slot_count):
            piece = tail_local[:, :, t, :].reshape(n_tail, tile)
            tail_pieces.append(lax.all_gather(piece, "col", axis=0))
        return after(tail_pieces[-1])

    sep_slots = -(-n_columns // n_row)
    get_panel = separator_panels(working[:sep_slots], n_row, n_col, n_columns, gather_tail)

    sep_factor = jnp.zeros((n_columns * tile, n_columns * tile), jnp.float32)
    tail_factor = jnp.zeros((n_tail, n_columns * tile), jnp.float32)
    for k in range(n_columns):
        panel = get_panel(k)
        tail_panel = tail_pieces[k // n_col][k % n_col]
        if k > 0:
            top = sep_factor[k * tile:(k + 1) * tile, : k * tile]
            panel = panel - mm(sep_factor[k * tile:, : k * tile], top.T, lax.Precision.HIGH)
            tail_panel = tail_panel - mm(tail_factor[:, : k * tile], top.T, lax.Precision.HIGH)
        diag = panel[:tile]
        diag = jnp.tril(diag) + jnp.tril(diag, -1).T
        lkk, linv = factor_diag(diag)
        if k + 1 < n_columns:
            block = jnp.concatenate([lkk, mm(panel[tile:], linv.T)], axis=0)
        else:
            block = lkk
        sep_factor = lax.dynamic_update_slice(sep_factor, block, (k * tile, k * tile))
        tail_factor = lax.dynamic_update_slice(tail_factor, mm(tail_panel, linv.T), (0, k * tile))

    outs = []
    for slot in range(slot_count):
        tile_row = slot * n_row + row_at
        start = jnp.minimum(tile_row, n_columns - 1) * tile
        picked = lax.dynamic_slice_in_dim(sep_factor, start, tile, axis=0)
        if slot >= tail_first:
            tail_rows = tail_factor[(slot - tail_first) * tile:(slot - tail_first + 1) * tile]
            picked = jnp.where(tile_row < n_columns, picked, tail_rows)
        picked = picked.reshape(tile, col_slot_count, n_col, tile)
        picked = lax.dynamic_index_in_dim(picked, col_at, axis=2, keepdims=False)
        outs.append(picked)
    return jnp.stack(outs, axis=0)


def solution(mesh):
    in_specs = (P(None, "row", None, "col"), P(None, "row"), P(None, "col"))
    out_specs = P(None, "row", None, "col")
    return jax.shard_map(shards, mesh=mesh, in_specs=in_specs, out_specs=out_specs, check_vma=False)
```

```python
import jax
import jax.numpy as jnp
from jax import lax
from jax.sharding import PartitionSpec as P

HIGHEST = lax.Precision.HIGHEST


def mm(a, b, precision=HIGHEST):
    return jnp.dot(a, b, precision=precision, preferred_element_type=jnp.float32)


def separator_panels(sep_local, n_row, n_col, n_columns, after_first):
    sep_slots, tile, cslots, _ = sep_local.shape
    if sep_slots == 1 and n_row == n_columns:
        pieces = []
        for t in range(cslots):
            piece = sep_local[0, :, t, :]
            if t == 1:
                piece = piece + after_first(pieces[0])
            pieces.append(lax.all_gather(piece, ("col", "row"), axis=0))
        if cslots == 1:
            after_first(pieces[0])

        def panel(k):
            base = (k % n_col) * n_row
            return pieces[k // n_col][base + k:base + n_row].reshape((n_columns - k) * tile, tile)

        return panel
    after_first(None)
    g = lax.all_gather(sep_local, "row", axis=1, tiled=True)
    g = g.reshape(sep_slots * n_row * tile, cslots, tile)[: n_columns * tile]
    g = lax.all_gather(g, "col", axis=2)

    def panel(k):
        return g[k * tile:, k // n_col, k % n_col, :]

    return panel


def after(value):
    return value.reshape(-1)[0] * 0.0


def lower_inverse(lower):
    size = lower.shape[0]
    eye = jnp.eye(size, dtype=lower.dtype)
    diag = jnp.sum(lower * eye, axis=1)
    strict = jnp.tril(jnp.ones((size, size), jnp.bool_), -1)
    power = jnp.where(strict, -lower / diag[:, None], 0.0)
    product = eye + power
    span = 2
    while span < size:
        power = mm(power, power)
        product = mm(product, eye + power)
        span *= 2
    return product / diag[None, :]


def factor_diag(diag):
    half = diag.shape[0] // 2
    l00 = jnp.tril(lax.linalg.cholesky(diag[:half, :half], symmetrize_input=False))
    i00 = lower_inverse(l00)
    l10 = mm(diag[half:, :half], i00.T)
    s11 = diag[half:, half:] - mm(l10, l10.T)
    l11 = jnp.tril(lax.linalg.cholesky(s11, symmetrize_input=True))
    i11 = lower_inverse(l11)
    i10 = -mm(i11, mm(l10, i00))
    zero = jnp.zeros((half, half), diag.dtype)
    lkk = jnp.block([[l00, zero], [l10, l11]])
    linv = jnp.block([[i00, zero], [i10, i11]])
    return lkk, linv


def shards(front_tiles, lead_tiles, damping):
    slot_count, tile, col_slot_count, _ = front_tiles.shape
    n_row = lax.axis_size("row")
    n_col = lax.axis_size("col")
    row_at = lax.axis_index("row")
    col_at = lax.axis_index("col")
    n_columns = col_slot_count * n_col
    row_tiles = jnp.arange(slot_count, dtype=jnp.int32) * n_row + row_at
    col_tiles = jnp.arange(col_slot_count, dtype=jnp.int32) * n_col + col_at
    leads = jnp.where(row_tiles < n_columns, 0, lead_tiles[:, 0])
    kept_mask = col_tiles[None, :] >= leads[:, None]
    working = jnp.where(kept_mask[:, None, :, None], front_tiles, 0.0)
    identity = jnp.eye(tile, dtype=jnp.float32)
    on_diagonal = (row_tiles[:, None] == col_tiles[None, :])[:, None, :, None]
    damp_term = identity[None, :, None, :] * damping[None, None, :, :]
    working = working + jnp.where(on_diagonal, damp_term, 0.0)

    tail_first = n_columns // n_row
    n_tail = (slot_count - tail_first) * tile
    tail_pieces = []
    tail_sources = []

    def gather_tail(first_piece):
        tail_local = working[tail_first:]
        if first_piece is not None:
            tail_local = tail_local + after(first_piece)
        tail_sources.append(tail_local)
        for t in range(col_slot_count):
            piece = tail_local[:, :, t, :].reshape(n_tail, tile)
            tail_pieces.append(lax.all_gather(piece, "col", axis=0))
        return after(tail_pieces[-1])

    sep_slots = -(-n_columns // n_row)
    get_panel = separator_panels(working[:sep_slots], n_row, n_col, n_columns, gather_tail)

    total_rows = n_columns * tile + n_tail
    factor = jnp.zeros((total_rows, n_columns * tile), jnp.float32)
    for k in range(n_columns):
        cols = slice(k * tile, (k + 1) * tile)
        panel = jnp.concatenate([get_panel(k), tail_pieces[k // n_col][k % n_col]], axis=0)
        if k > 0:
            left = factor[k * tile:, : k * tile]
            top = factor[k * tile:(k + 1) * tile, : k * tile]
            panel = panel - mm(left, top.T, lax.Precision.HIGH)
        diag = panel[:tile]
        if k == 0:
            diag = diag + after(tail_sources[0])
        diag = jnp.tril(diag) + jnp.tril(diag, -1).T
        lkk, linv = factor_diag(diag)
        below = mm(panel[tile:], linv.T)
        factor = lax.dynamic_update_slice(factor, jnp.concatenate([lkk, below], axis=0), (k * tile, k * tile))

    outs = []
    for slot in range(slot_count):
        tile_row = slot * n_row + row_at
        if slot < tail_first:
            start = tile_row * tile
        else:
            tail_start = n_columns * tile + (slot - tail_first) * tile
            start = jnp.where(tile_row < n_columns, tile_row * tile, tail_start)
        picked = lax.dynamic_slice_in_dim(factor, start, tile, axis=0)
        picked = picked.reshape(tile, col_slot_count, n_col, tile)
        picked = lax.dynamic_index_in_dim(picked, col_at, axis=2, keepdims=False)
        outs.append(picked)
    return jnp.stack(outs, axis=0)


def solution(mesh):
    in_specs = (P(None, "row", None, "col"), P(None, "row"), P(None, "col"))
    out_specs = P(None, "row", None, "col")
    return jax.shard_map(shards, mesh=mesh, in_specs=in_specs, out_specs=out_specs, check_vma=False)
```

```python
import jax
import jax.numpy as jnp
from jax import lax
from jax.sharding import PartitionSpec as P

HIGHEST = lax.Precision.HIGHEST


def mm(a, b, precision=HIGHEST):
    return jnp.dot(a, b, precision=precision, preferred_element_type=jnp.float32)


def separator_panels(sep_local, n_row, n_col, n_columns, after_first):
    sep_slots, tile, cslots, _ = sep_local.shape
    if sep_slots == 1 and n_row == n_columns:
        pieces = []
        for t in range(cslots):
            piece = sep_local[0, :, t, :]
            if t == 1:
                piece = piece + after_first(pieces[0])
            pieces.append(lax.all_gather(piece, ("col", "row"), axis=0))
        if cslots == 1:
            after_first(pieces[0])

        def panel(k):
            base = (k % n_col) * n_row
            return pieces[k // n_col][base + k:base + n_row].reshape((n_columns - k) * tile, tile)

        return panel
    after_first(None)
    g = lax.all_gather(sep_local, "row", axis=1, tiled=True)
    g = g.reshape(sep_slots * n_row * tile, cslots, tile)[: n_columns * tile]
    g = lax.all_gather(g, "col", axis=2)

    def panel(k):
        return g[k * tile:, k // n_col, k % n_col, :]

    return panel


def after(value):
    return value.reshape(-1)[0] * 0.0


def lower_inverse(lower):
    size = lower.shape[0]
    eye = jnp.eye(size, dtype=lower.dtype)
    diag = jnp.sum(lower * eye, axis=1)
    strict = jnp.tril(jnp.ones((size, size), jnp.bool_), -1)
    power = jnp.where(strict, -lower / diag[:, None], 0.0)
    product = eye
    covered = 1
    while covered < size:
        both = mm(jnp.concatenate([product, power], axis=0), eye + power)
        product = both[:size]
        power = both[size:] - power
        covered *= 2
    return product / diag[None, :]


def factor_diag(diag):
    half = diag.shape[0] // 2
    l00 = jnp.tril(lax.linalg.cholesky(diag[:half, :half], symmetrize_input=False))
    i00 = lower_inverse(l00)
    l10 = mm(diag[half:, :half], i00.T)
    s11 = diag[half:, half:] - mm(l10, l10.T)
    l11 = jnp.tril(lax.linalg.cholesky(s11, symmetrize_input=True))
    i11 = lower_inverse(l11)
    i10 = -mm(i11, mm(l10, i00))
    zero = jnp.zeros((half, half), diag.dtype)
    lkk = jnp.block([[l00, zero], [l10, l11]])
    linv = jnp.block([[i00, zero], [i10, i11]])
    return lkk, linv


def shards(front_tiles, lead_tiles, damping):
    slot_count, tile, col_slot_count, _ = front_tiles.shape
    n_row = lax.axis_size("row")
    n_col = lax.axis_size("col")
    row_at = lax.axis_index("row")
    col_at = lax.axis_index("col")
    n_columns = col_slot_count * n_col
    row_tiles = jnp.arange(slot_count, dtype=jnp.int32) * n_row + row_at
    col_tiles = jnp.arange(col_slot_count, dtype=jnp.int32) * n_col + col_at
    leads = jnp.where(row_tiles < n_columns, 0, lead_tiles[:, 0])
    kept_mask = col_tiles[None, :] >= leads[:, None]
    working = jnp.where(kept_mask[:, None, :, None], front_tiles, 0.0)
    identity = jnp.eye(tile, dtype=jnp.float32)
    on_diagonal = (row_tiles[:, None] == col_tiles[None, :])[:, None, :, None]
    damp_term = identity[None, :, None, :] * damping[None, None, :, :]
    working = working + jnp.where(on_diagonal, damp_term, 0.0)

    tail_first = n_columns // n_row
    n_tail = (slot_count - tail_first) * tile
    tail_pieces = []
    tail_sources = []

    def gather_tail(first_piece):
        tail_local = working[tail_first:]
        if first_piece is not None:
            tail_local = tail_local + after(first_piece)
        tail_sources.append(tail_local)
        for t in range(col_slot_count):
            piece = tail_local[:, :, t, :].reshape(n_tail, tile)
            tail_pieces.append(lax.all_gather(piece, "col", axis=0))
        return after(tail_pieces[-1])

    sep_slots = -(-n_columns // n_row)
    get_panel = separator_panels(working[:sep_slots], n_row, n_col, n_columns, gather_tail)

    total_rows = n_columns * tile + n_tail
    factor = jnp.zeros((total_rows, n_columns * tile), jnp.float32)
    for k in range(n_columns):
        cols = slice(k * tile, (k + 1) * tile)
        panel = jnp.concatenate([get_panel(k), tail_pieces[k // n_col][k % n_col]], axis=0)
        if k > 0:
            left = factor[k * tile:, : k * tile]
            top = factor[k * tile:(k + 1) * tile, : k * tile]
            panel = panel - mm(left, top.T, lax.Precision.HIGH)
        diag = panel[:tile]
        if k == 0:
            diag = diag + after(tail_sources[0])
        diag = jnp.tril(diag) + jnp.tril(diag, -1).T
        lkk, linv = factor_diag(diag)
        below = mm(panel[tile:], linv.T)
        factor = factor.at[k * tile:, cols].set(jnp.concatenate([lkk, below], axis=0))

    outs = []
    for slot in range(slot_count):
        tile_row = slot * n_row + row_at
        if slot < tail_first:
            start = tile_row * tile
        else:
            tail_start = n_columns * tile + (slot - tail_first) * tile
            start = jnp.where(tile_row < n_columns, tile_row * tile, tail_start)
        picked = lax.dynamic_slice_in_dim(factor, start, tile, axis=0)
        picked = picked.reshape(tile, col_slot_count, n_col, tile)
        picked = lax.dynamic_index_in_dim(picked, col_at, axis=2, keepdims=False)
        outs.append(picked)
    return jnp.stack(outs, axis=0)


def solution(mesh):
    in_specs = (P(None, "row", None, "col"), P(None, "row"), P(None, "col"))
    out_specs = P(None, "row", None, "col")
    return jax.shard_map(shards, mesh=mesh, in_specs=in_specs, out_specs=out_specs, check_vma=False)
```

```python
import jax
import jax.numpy as jnp
from jax import lax
from jax.sharding import PartitionSpec as P

HIGHEST = lax.Precision.HIGHEST


def mm(a, b, precision=HIGHEST):
    return jnp.dot(a, b, precision=precision, preferred_element_type=jnp.float32)


def separator_panels(sep_local, n_row, n_col, n_columns, after_first):
    sep_slots, tile, cslots, _ = sep_local.shape
    if sep_slots == 1 and n_row == n_columns:
        pieces = []
        for t in range(cslots):
            piece = sep_local[0, :, t, :]
            if t == 1:
                piece = piece + after_first(pieces[0])
            pieces.append(lax.all_gather(piece, ("col", "row"), axis=0))
        if cslots == 1:
            after_first(pieces[0])

        def panel(k):
            base = (k % n_col) * n_row
            return pieces[k // n_col][base + k:base + n_row].reshape((n_columns - k) * tile, tile)

        return panel
    after_first(None)
    g = lax.all_gather(sep_local, "row", axis=1, tiled=True)
    g = g.reshape(sep_slots * n_row * tile, cslots, tile)[: n_columns * tile]
    g = lax.all_gather(g, "col", axis=2)

    def panel(k):
        return g[k * tile:, k // n_col, k % n_col, :]

    return panel


def after(value):
    return value.reshape(-1)[0] * 0.0


def lower_inverse(lower):
    size = lower.shape[0]
    eye = jnp.eye(size, dtype=lower.dtype)
    diag = jnp.sum(lower * eye, axis=1)
    strict = jnp.tril(jnp.ones((size, size), jnp.bool_), -1)
    power = jnp.where(strict, -lower / diag[:, None], 0.0)
    product = eye
    covered = 1
    while covered < size:
        both = mm(jnp.concatenate([product, power], axis=0), eye + power)
        product = both[:size]
        power = both[size:] - power
        covered *= 2
    return product / diag[None, :]


def factor_diag(diag):
    half = diag.shape[0] // 2
    l00 = jnp.tril(lax.linalg.cholesky(diag[:half, :half], symmetrize_input=False))
    i00 = lower_inverse(l00)
    l10 = mm(diag[half:, :half], i00.T)
    s11 = diag[half:, half:] - mm(l10, l10.T)
    l11 = jnp.tril(lax.linalg.cholesky(s11, symmetrize_input=True))
    i11 = lower_inverse(l11)
    i10 = -mm(i11, mm(l10, i00))
    zero = jnp.zeros((half, half), diag.dtype)
    lkk = jnp.block([[l00, zero], [l10, l11]])
    linv = jnp.block([[i00, zero], [i10, i11]])
    return lkk, linv


def shards(front_tiles, lead_tiles, damping):
    slot_count, tile, col_slot_count, _ = front_tiles.shape
    n_row = lax.axis_size("row")
    n_col = lax.axis_size("col")
    row_at = lax.axis_index("row")
    col_at = lax.axis_index("col")
    n_columns = col_slot_count * n_col
    row_tiles = jnp.arange(slot_count, dtype=jnp.int32) * n_row + row_at
    col_tiles = jnp.arange(col_slot_count, dtype=jnp.int32) * n_col + col_at
    leads = jnp.where(row_tiles < n_columns, 0, lead_tiles[:, 0])
    kept_mask = col_tiles[None, :] >= leads[:, None]
    working = jnp.where(kept_mask[:, None, :, None], front_tiles, 0.0)
    identity = jnp.eye(tile, dtype=jnp.float32)
    on_diagonal = (row_tiles[:, None] == col_tiles[None, :])[:, None, :, None]
    damp_term = identity[None, :, None, :] * damping[None, None, :, :]
    working = working + jnp.where(on_diagonal, damp_term, 0.0)

    tail_first = n_columns // n_row
    n_tail = (slot_count - tail_first) * tile
    tail_pieces = []
    tail_sources = []

    def gather_tail(first_piece):
        tail_local = working[tail_first:]
        if first_piece is not None:
            tail_local = tail_local + after(first_piece)
        tail_sources.append(tail_local)
        for t in range(col_slot_count):
            piece = tail_local[:, :, t, :].reshape(n_tail, tile)
            tail_pieces.append(lax.all_gather(piece, "col", axis=0))
        return after(tail_pieces[-1])

    sep_slots = -(-n_columns // n_row)
    get_panel = separator_panels(working[:sep_slots], n_row, n_col, n_columns, gather_tail)

    total_rows = n_columns * tile + n_tail
    factor = jnp.zeros((total_rows, n_columns * tile), jnp.float32)
    for k in range(n_columns):
        cols = slice(k * tile, (k + 1) * tile)
        panel = jnp.concatenate([get_panel(k), tail_pieces[k // n_col][k % n_col]], axis=0)
        if k > 0:
            left = factor[k * tile:, : k * tile]
            top = factor[k * tile:(k + 1) * tile, : k * tile]
            panel = panel - mm(left, top.T, lax.Precision.HIGH)
        diag = panel[:tile]
        if k == 0:
            diag = diag + after(tail_sources[0])
        diag = jnp.tril(diag) + jnp.tril(diag, -1).T
        lkk, linv = factor_diag(diag)
        below = mm(panel[tile:], linv.T, lax.Precision.HIGH)
        factor = factor.at[k * tile:, cols].set(jnp.concatenate([lkk, below], axis=0))

    outs = []
    for slot in range(slot_count):
        tile_row = slot * n_row + row_at
        if slot < tail_first:
            start = tile_row * tile
        else:
            tail_start = n_columns * tile + (slot - tail_first) * tile
            start = jnp.where(tile_row < n_columns, tile_row * tile, tail_start)
        picked = lax.dynamic_slice_in_dim(factor, start, tile, axis=0)
        picked = picked.reshape(tile, col_slot_count, n_col, tile)
        picked = lax.dynamic_index_in_dim(picked, col_at, axis=2, keepdims=False)
        outs.append(picked)
    return jnp.stack(outs, axis=0)


def solution(mesh):
    in_specs = (P(None, "row", None, "col"), P(None, "row"), P(None, "col"))
    out_specs = P(None, "row", None, "col")
    return jax.shard_map(shards, mesh=mesh, in_specs=in_specs, out_specs=out_specs, check_vma=False)
```

```python
import jax
import jax.numpy as jnp
from jax import lax
from jax.sharding import PartitionSpec as P

HIGHEST = lax.Precision.HIGHEST


def mm(a, b, precision=HIGHEST):
    return jnp.dot(a, b, precision=precision, preferred_element_type=jnp.float32)


def separator_panels(sep_local, n_row, n_col, n_columns, after_first):
    sep_slots, tile, cslots, _ = sep_local.shape
    if sep_slots == 1 and n_row == n_columns:
        pieces = []
        previous = None
        for t in range(cslots):
            piece = sep_local[0, :, t, :] + after_first(t, previous)
            pieces.append(lax.all_gather(piece, ("col", "row"), axis=0))
            previous = after(pieces[-1])

        def panel(k):
            base = (k % n_col) * n_row
            return pieces[k // n_col][base + k:base + n_row].reshape((n_columns - k) * tile, tile)

        return panel
    for t in range(cslots):
        after_first(t, None)
    g = lax.all_gather(sep_local, "row", axis=1, tiled=True)
    g = g.reshape(sep_slots * n_row * tile, cslots, tile)[: n_columns * tile]
    g = lax.all_gather(g, "col", axis=2)

    def panel(k):
        return g[k * tile:, k // n_col, k % n_col, :]

    return panel


def after(value):
    return value.reshape(-1)[0] * 0.0


def lower_inverse(lower):
    size = lower.shape[0]
    eye = jnp.eye(size, dtype=lower.dtype)
    diag = jnp.sum(lower * eye, axis=1)
    strict = jnp.tril(jnp.ones((size, size), jnp.bool_), -1)
    power = jnp.where(strict, -lower / diag[:, None], 0.0)
    product = eye
    covered = 1
    while covered < size:
        both = mm(jnp.concatenate([product, power], axis=0), eye + power)
        product = both[:size]
        power = both[size:] - power
        covered *= 2
    return product / diag[None, :]


def factor_diag(diag):
    half = diag.shape[0] // 2
    l00 = jnp.tril(lax.linalg.cholesky(diag[:half, :half], symmetrize_input=False))
    i00 = lower_inverse(l00)
    l10 = mm(diag[half:, :half], i00.T)
    s11 = diag[half:, half:] - mm(l10, l10.T)
    l11 = jnp.tril(lax.linalg.cholesky(s11, symmetrize_input=True))
    i11 = lower_inverse(l11)
    i10 = -mm(i11, mm(l10, i00))
    zero = jnp.zeros((half, half), diag.dtype)
    lkk = jnp.block([[l00, zero], [l10, l11]])
    linv = jnp.block([[i00, zero], [i10, i11]])
    return lkk, linv


def shards(front_tiles, lead_tiles, damping):
    slot_count, tile, col_slot_count, _ = front_tiles.shape
    n_row = lax.axis_size("row")
    n_col = lax.axis_size("col")
    row_at = lax.axis_index("row")
    col_at = lax.axis_index("col")
    n_columns = col_slot_count * n_col
    row_tiles = jnp.arange(slot_count, dtype=jnp.int32) * n_row + row_at
    col_tiles = jnp.arange(col_slot_count, dtype=jnp.int32) * n_col + col_at
    leads = jnp.where(row_tiles < n_columns, 0, lead_tiles[:, 0])
    kept_mask = col_tiles[None, :] >= leads[:, None]
    working = jnp.where(kept_mask[:, None, :, None], front_tiles, 0.0)
    identity = jnp.eye(tile, dtype=jnp.float32)
    on_diagonal = (row_tiles[:, None] == col_tiles[None, :])[:, None, :, None]
    damp_term = identity[None, :, None, :] * damping[None, None, :, :]
    working = working + jnp.where(on_diagonal, damp_term, 0.0)

    tail_first = n_columns // n_row
    n_tail = (slot_count - tail_first) * tile
    tail_pieces = []

    def gather_tail(t, dependency):
        piece = working[tail_first:, :, t, :].reshape(n_tail, tile)
        if dependency is not None:
            piece = piece + dependency
        tail_pieces.append(lax.all_gather(piece, "col", axis=0))
        return after(tail_pieces[-1])

    sep_slots = -(-n_columns // n_row)
    get_panel = separator_panels(working[:sep_slots], n_row, n_col, n_columns, gather_tail)

    total_rows = n_columns * tile + n_tail
    factor = jnp.zeros((total_rows, n_columns * tile), jnp.float32)
    for k in range(n_columns):
        cols = slice(k * tile, (k + 1) * tile)
        panel = jnp.concatenate([get_panel(k), tail_pieces[k // n_col][k % n_col]], axis=0)
        if k > 0:
            left = factor[k * tile:, : k * tile]
            top = factor[k * tile:(k + 1) * tile, : k * tile]
            panel = panel - mm(left, top.T, lax.Precision.HIGH)
        diag = panel[:tile]
        diag = jnp.tril(diag) + jnp.tril(diag, -1).T
        lkk, linv = factor_diag(diag)
        below = mm(panel[tile:], linv.T)
        factor = factor.at[k * tile:, cols].set(jnp.concatenate([lkk, below], axis=0))

    outs = []
    for slot in range(slot_count):
        tile_row = slot * n_row + row_at
        if slot < tail_first:
            start = tile_row * tile
        else:
            tail_start = n_columns * tile + (slot - tail_first) * tile
            start = jnp.where(tile_row < n_columns, tile_row * tile, tail_start)
        picked = lax.dynamic_slice_in_dim(factor, start, tile, axis=0)
        picked = picked.reshape(tile, col_slot_count, n_col, tile)
        picked = lax.dynamic_index_in_dim(picked, col_at, axis=2, keepdims=False)
        outs.append(picked)
    return jnp.stack(outs, axis=0)


def solution(mesh):
    in_specs = (P(None, "row", None, "col"), P(None, "row"), P(None, "col"))
    out_specs = P(None, "row", None, "col")
    return jax.shard_map(shards, mesh=mesh, in_specs=in_specs, out_specs=out_specs, check_vma=False)
```

```python
import jax
import jax.numpy as jnp
from jax import lax
from jax.sharding import PartitionSpec as P

HIGHEST = lax.Precision.HIGHEST


def mm(a, b, precision=HIGHEST):
    return jnp.dot(a, b, precision=precision, preferred_element_type=jnp.float32)


def separator_panels(sep_local, n_row, n_col, n_columns, after_first):
    sep_slots, tile, cslots, _ = sep_local.shape
    if sep_slots == 1 and n_row == n_columns:
        pieces = []
        for t in range(cslots):
            piece = sep_local[0, :, t, :]
            if t == 1:
                piece = piece + after_first(pieces[0])
            pieces.append(lax.all_gather(piece, ("col", "row"), axis=0))
        if cslots == 1:
            after_first(pieces[0])

        def panel(k):
            base = (k % n_col) * n_row
            return pieces[k // n_col][base + k:base + n_row].reshape((n_columns - k) * tile, tile)

        return panel
    after_first(None)
    g = lax.all_gather(sep_local, "row", axis=1, tiled=True)
    g = g.reshape(sep_slots * n_row * tile, cslots, tile)[: n_columns * tile]
    g = lax.all_gather(g, "col", axis=2)

    def panel(k):
        return g[k * tile:, k // n_col, k % n_col, :]

    return panel


def after(value):
    return value.reshape(-1)[0] * 0.0


def lower_inverse(lower):
    size = lower.shape[0]
    eye = jnp.eye(size, dtype=lower.dtype)
    diag = jnp.sum(lower * eye, axis=1)
    strict = jnp.tril(jnp.ones((size, size), jnp.bool_), -1)
    power = jnp.where(strict, -lower / diag[:, None], 0.0)
    product = eye
    covered = 1
    while covered < size:
        both = mm(jnp.concatenate([product, power], axis=0), eye + power)
        product = both[:size]
        power = both[size:] - power
        covered *= 2
    return product / diag[None, :]


def factor_diag(diag):
    half = diag.shape[0] // 2
    l00 = jnp.tril(lax.linalg.cholesky(diag[:half, :half], symmetrize_input=False))
    i00 = lower_inverse(l00)
    l10 = mm(diag[half:, :half], i00.T)
    s11 = diag[half:, half:] - mm(l10, l10.T)
    l11 = jnp.tril(lax.linalg.cholesky(s11, symmetrize_input=True))
    i11 = lower_inverse(l11)
    i10 = -mm(i11, mm(l10, i00))
    zero = jnp.zeros((half, half), diag.dtype)
    lkk = jnp.block([[l00, zero], [l10, l11]])
    linv = jnp.block([[i00, zero], [i10, i11]])
    return lkk, linv


def shards(front_tiles, lead_tiles, damping):
    slot_count, tile, col_slot_count, _ = front_tiles.shape
    n_row = lax.axis_size("row")
    n_col = lax.axis_size("col")
    row_at = lax.axis_index("row")
    col_at = lax.axis_index("col")
    n_columns = col_slot_count * n_col
    row_tiles = jnp.arange(slot_count, dtype=jnp.int32) * n_row + row_at
    col_tiles = jnp.arange(col_slot_count, dtype=jnp.int32) * n_col + col_at
    leads = jnp.where(row_tiles < n_columns, 0, lead_tiles[:, 0])
    kept_mask = col_tiles[None, :] >= leads[:, None]
    working = jnp.where(kept_mask[:, None, :, None], front_tiles, 0.0)
    identity = jnp.eye(tile, dtype=jnp.float32)
    on_diagonal = (row_tiles[:, None] == col_tiles[None, :])[:, None, :, None]
    damp_term = identity[None, :, None, :] * damping[None, None, :, :]
    working = working + jnp.where(on_diagonal, damp_term, 0.0)

    tail_first = n_columns // n_row
    n_tail = (slot_count - tail_first) * tile
    tail_pieces = []
    tail_sources = []

    def gather_tail(first_piece):
        tail_local = working[tail_first:]
        if first_piece is not None:
            tail_local = tail_local + after(first_piece)
        tail_sources.append(tail_local)
        for t in range(col_slot_count):
            piece = tail_local[:, :, t, :].reshape(n_tail, tile)
            tail_pieces.append(lax.all_gather(piece, "col", axis=0))
        return after(tail_pieces[-1])

    sep_slots = -(-n_columns // n_row)
    get_panel = separator_panels(working[:sep_slots], n_row, n_col, n_columns, gather_tail)

    total_rows = n_columns * tile + n_tail
    factor = jnp.zeros((total_rows, n_columns * tile), jnp.float32)
    for k in range(n_columns):
        cols = slice(k * tile, (k + 1) * tile)
        if k == 0:
            panel = get_panel(k)
        else:
            panel = jnp.concatenate([get_panel(k), tail_pieces[k // n_col][k % n_col]], axis=0)
        if k > 0:
            left = factor[k * tile:, : k * tile]
            top = factor[k * tile:(k + 1) * tile, : k * tile]
            panel = panel - mm(left, top.T, lax.Precision.HIGH)
        diag = panel[:tile]
        if k == 0:
            diag = diag + after(tail_sources[0])
        diag = jnp.tril(diag) + jnp.tril(diag, -1).T
        lkk, linv = factor_diag(diag)
        below = mm(panel[tile:], linv.T)
        if k == 0:
            factor = lax.dynamic_update_slice(factor, jnp.concatenate([lkk, below], axis=0), (0, 0))
            tail_below = mm(tail_pieces[0][0], linv.T)
            factor = lax.dynamic_update_slice(factor, tail_below, (n_columns * tile, 0))
        else:
            factor = factor.at[k * tile:, cols].set(jnp.concatenate([lkk, below], axis=0))

    outs = []
    for slot in range(slot_count):
        tile_row = slot * n_row + row_at
        if slot < tail_first:
            start = tile_row * tile
        else:
            tail_start = n_columns * tile + (slot - tail_first) * tile
            start = jnp.where(tile_row < n_columns, tile_row * tile, tail_start)
        picked = lax.dynamic_slice_in_dim(factor, start, tile, axis=0)
        picked = picked.reshape(tile, col_slot_count, n_col, tile)
        picked = lax.dynamic_index_in_dim(picked, col_at, axis=2, keepdims=False)
        outs.append(picked)
    return jnp.stack(outs, axis=0)


def solution(mesh):
    in_specs = (P(None, "row", None, "col"), P(None, "row"), P(None, "col"))
    out_specs = P(None, "row", None, "col")
    return jax.shard_map(shards, mesh=mesh, in_specs=in_specs, out_specs=out_specs, check_vma=False)
```

```python
import jax
import jax.numpy as jnp
from jax import lax
from jax.sharding import PartitionSpec as P

HIGHEST = lax.Precision.HIGHEST


def mm(a, b, precision=HIGHEST):
    return jnp.dot(a, b, precision=precision, preferred_element_type=jnp.float32)


def separator_panels(sep_local, n_row, n_col, n_columns, after_first):
    sep_slots, tile, cslots, _ = sep_local.shape
    if sep_slots == 1 and n_row == n_columns:
        pieces = []
        for t in range(cslots):
            piece = sep_local[0, :, t, :]
            if t == 1:
                piece = piece + after_first(pieces[0])
            pieces.append(lax.all_gather(piece, ("col", "row"), axis=0))
        if cslots == 1:
            after_first(pieces[0])

        def panel(k):
            base = (k % n_col) * n_row
            return pieces[k // n_col][base + k:base + n_row].reshape((n_columns - k) * tile, tile)

        return panel
    after_first(None)
    g = lax.all_gather(sep_local, "row", axis=1, tiled=True)
    g = g.reshape(sep_slots * n_row * tile, cslots, tile)[: n_columns * tile]
    g = lax.all_gather(g, "col", axis=2)

    def panel(k):
        return g[k * tile:, k // n_col, k % n_col, :]

    return panel


def after(value):
    return value.reshape(-1)[0] * 0.0


def lower_inverse(lower):
    size = lower.shape[0]
    eye = jnp.eye(size, dtype=lower.dtype)
    diag = jnp.sum(lower * eye, axis=1)
    strict = jnp.tril(jnp.ones((size, size), jnp.bool_), -1)
    power = jnp.where(strict, -lower / diag[:, None], 0.0)
    product = eye
    covered = 1
    while covered < size:
        both = mm(jnp.concatenate([product, power], axis=0), eye + power)
        product = both[:size]
        power = both[size:] - power
        covered *= 2
    return product / diag[None, :]


def factor_diag(diag):
    half = diag.shape[0] // 2
    l00 = jnp.tril(lax.linalg.cholesky(diag[:half, :half], symmetrize_input=False))
    i00 = lower_inverse(l00)
    l10 = mm(diag[half:, :half], i00.T)
    s11 = diag[half:, half:] - mm(l10, l10.T)
    l11 = jnp.tril(lax.linalg.cholesky(s11, symmetrize_input=True))
    i11 = lower_inverse(l11)
    i10 = -mm(i11, mm(l10, i00))
    zero = jnp.zeros((half, half), diag.dtype)
    lkk = jnp.block([[l00, zero], [l10, l11]])
    linv = jnp.block([[i00, zero], [i10, i11]])
    return lkk, linv


def shards(front_tiles, lead_tiles, damping):
    slot_count, tile, col_slot_count, _ = front_tiles.shape
    n_row = lax.axis_size("row")
    n_col = lax.axis_size("col")
    row_at = lax.axis_index("row")
    col_at = lax.axis_index("col")
    n_columns = col_slot_count * n_col
    row_tiles = jnp.arange(slot_count, dtype=jnp.int32) * n_row + row_at
    col_tiles = jnp.arange(col_slot_count, dtype=jnp.int32) * n_col + col_at
    leads = jnp.where(row_tiles < n_columns, 0, lead_tiles[:, 0])
    kept_mask = col_tiles[None, :] >= leads[:, None]
    working = jnp.where(kept_mask[:, None, :, None], front_tiles, 0.0)
    identity = jnp.eye(tile, dtype=jnp.float32)
    on_diagonal = (row_tiles[:, None] == col_tiles[None, :])[:, None, :, None]
    damp_term = identity[None, :, None, :] * damping[None, None, :, :]
    working = working + jnp.where(on_diagonal, damp_term, 0.0)

    tail_first = n_columns // n_row
    n_tail = (slot_count - tail_first) * tile
    tail_pieces = []
    tail_sources = []

    def gather_tail(first_piece):
        tail_local = working[tail_first:]
        if first_piece is not None:
            tail_local = tail_local + after(first_piece)
        tail_sources.append(tail_local)
        for t in range(col_slot_count):
            piece = tail_local[:, :, t, :].reshape(n_tail, tile)
            tail_pieces.append(lax.all_gather(piece, "col", axis=0))
        return after(tail_pieces[0])

    sep_slots = -(-n_columns // n_row)
    get_panel = separator_panels(working[:sep_slots], n_row, n_col, n_columns, gather_tail)

    total_rows = n_columns * tile + n_tail
    factor = jnp.zeros((total_rows, n_columns * tile), jnp.float32)
    for k in range(n_columns):
        cols = slice(k * tile, (k + 1) * tile)
        if k == 0:
            panel = get_panel(k)
        else:
            panel = jnp.concatenate([get_panel(k), tail_pieces[k // n_col][k % n_col]], axis=0)
        if k > 0:
            left = factor[k * tile:, : k * tile]
            top = factor[k * tile:(k + 1) * tile, : k * tile]
            panel = panel - mm(left, top.T, lax.Precision.HIGH)
        diag = panel[:tile]
        if k == 0:
            diag = diag + after(tail_sources[0])
        diag = jnp.tril(diag) + jnp.tril(diag, -1).T
        lkk, linv = factor_diag(diag)
        below = mm(panel[tile:], linv.T)
        if k == 0:
            factor = lax.dynamic_update_slice(factor, jnp.concatenate([lkk, below], axis=0), (0, 0))
            tail_below = mm(tail_pieces[0][0], linv.T)
            factor = lax.dynamic_update_slice(factor, tail_below, (n_columns * tile, 0))
        else:
            factor = factor.at[k * tile:, cols].set(jnp.concatenate([lkk, below], axis=0))

    outs = []
    for slot in range(slot_count):
        tile_row = slot * n_row + row_at
        if slot < tail_first:
            start = tile_row * tile
        else:
            tail_start = n_columns * tile + (slot - tail_first) * tile
            start = jnp.where(tile_row < n_columns, tile_row * tile, tail_start)
        picked = lax.dynamic_slice_in_dim(factor, start, tile, axis=0)
        picked = picked.reshape(tile, col_slot_count, n_col, tile)
        picked = lax.dynamic_index_in_dim(picked, col_at, axis=2, keepdims=False)
        outs.append(picked)
    return jnp.stack(outs, axis=0)


def solution(mesh):
    in_specs = (P(None, "row", None, "col"), P(None, "row"), P(None, "col"))
    out_specs = P(None, "row", None, "col")
    return jax.shard_map(shards, mesh=mesh, in_specs=in_specs, out_specs=out_specs, check_vma=False)
```

```python
import jax
import jax.numpy as jnp
from jax import lax
from jax.sharding import PartitionSpec as P

HIGHEST = lax.Precision.HIGHEST


def mm(a, b, precision=HIGHEST):
    return jnp.dot(a, b, precision=precision, preferred_element_type=jnp.float32)


def separator_panels(sep_local, n_row, n_col, n_columns, after_first):
    sep_slots, tile, cslots, _ = sep_local.shape
    if sep_slots == 1 and n_row == n_columns:
        pieces = []
        for t in range(cslots):
            piece = sep_local[0, :, t, :]
            if t == 1:
                piece = piece + after_first(pieces[0])
            pieces.append(lax.all_gather(piece, ("col", "row"), axis=0))
        if cslots == 1:
            after_first(pieces[0])

        def panel(k):
            base = (k % n_col) * n_row
            return pieces[k // n_col][base + k:base + n_row].reshape((n_columns - k) * tile, tile)

        return panel
    after_first(None)
    g = lax.all_gather(sep_local, "row", axis=1, tiled=True)
    g = g.reshape(sep_slots * n_row * tile, cslots, tile)[: n_columns * tile]
    g = lax.all_gather(g, "col", axis=2)

    def panel(k):
        return g[k * tile:, k // n_col, k % n_col, :]

    return panel


def after(value):
    return value.reshape(-1)[0] * 0.0


def lower_inverse(lower):
    size = lower.shape[0]
    eye = jnp.eye(size, dtype=lower.dtype)
    diag = jnp.sum(lower * eye, axis=1)
    strict = jnp.tril(jnp.ones((size, size), jnp.bool_), -1)
    power = jnp.where(strict, -lower / diag[:, None], 0.0)
    product = eye
    covered = 1
    while covered < size:
        both = mm(jnp.concatenate([product, power], axis=0), eye + power)
        product = both[:size]
        power = both[size:] - power
        covered *= 2
    return product / diag[None, :]


def factor_diag(diag):
    half = diag.shape[0] // 2
    l00 = jnp.tril(lax.linalg.cholesky(diag[:half, :half], symmetrize_input=False))
    i00 = lower_inverse(l00)
    l10 = mm(diag[half:, :half], i00.T)
    s11 = diag[half:, half:] - mm(l10, l10.T)
    l11 = jnp.tril(lax.linalg.cholesky(s11, symmetrize_input=True))
    i11 = lower_inverse(l11)
    i10 = -mm(i11, mm(l10, i00))
    zero = jnp.zeros((half, half), diag.dtype)
    lkk = jnp.block([[l00, zero], [l10, l11]])
    linv = jnp.block([[i00, zero], [i10, i11]])
    return lkk, linv


def shards(front_tiles, lead_tiles, damping):
    slot_count, tile, col_slot_count, _ = front_tiles.shape
    n_row = lax.axis_size("row")
    n_col = lax.axis_size("col")
    row_at = lax.axis_index("row")
    col_at = lax.axis_index("col")
    n_columns = col_slot_count * n_col
    row_tiles = jnp.arange(slot_count, dtype=jnp.int32) * n_row + row_at
    col_tiles = jnp.arange(col_slot_count, dtype=jnp.int32) * n_col + col_at
    leads = jnp.where(row_tiles < n_columns, 0, lead_tiles[:, 0])
    kept_mask = col_tiles[None, :] >= leads[:, None]
    working = jnp.where(kept_mask[:, None, :, None], front_tiles, 0.0)
    identity = jnp.eye(tile, dtype=jnp.float32)
    on_diagonal = (row_tiles[:, None] == col_tiles[None, :])[:, None, :, None]
    damp_term = identity[None, :, None, :] * damping[None, None, :, :]
    working = working + jnp.where(on_diagonal, damp_term, 0.0)

    tail_first = n_columns // n_row
    n_tail = (slot_count - tail_first) * tile
    tail_pieces = []
    tail_sources = []

    def gather_tail(first_piece):
        tail_local = working[tail_first:]
        if first_piece is not None:
            tail_local = tail_local + after(first_piece)
        tail_sources.append(tail_local)
        for t in range(col_slot_count):
            piece = tail_local[:, :, t, :].reshape(n_tail, tile)
            tail_pieces.append(lax.all_gather(piece, "col", axis=0))
        return after(tail_pieces[-1])

    sep_slots = -(-n_columns // n_row)
    get_panel = separator_panels(working[:sep_slots], n_row, n_col, n_columns, gather_tail)

    total_rows = n_columns * tile + n_tail
    for k in range(n_columns):
        cols = slice(k * tile, (k + 1) * tile)
        if k == 0:
            panel = get_panel(k)
        else:
            panel = jnp.concatenate([get_panel(k), tail_pieces[k // n_col][k % n_col]], axis=0)
        if k > 0:
            left = factor[k * tile:, : k * tile]
            top = factor[k * tile:(k + 1) * tile, : k * tile]
            panel = panel - mm(left, top.T, lax.Precision.HIGH)
        diag = panel[:tile]
        if k == 0:
            diag = diag + after(tail_sources[0])
        diag = jnp.tril(diag) + jnp.tril(diag, -1).T
        lkk, linv = factor_diag(diag)
        below = mm(panel[tile:], linv.T)
        if k == 0:
            tail_below = mm(tail_pieces[0][0], linv.T)
            first = jnp.concatenate([lkk, below, tail_below], axis=0)
            factor = jnp.pad(first, ((0, 0), (0, (n_columns - 1) * tile)))
        else:
            factor = factor.at[k * tile:, cols].set(jnp.concatenate([lkk, below], axis=0))

    outs = []
    for slot in range(slot_count):
        tile_row = slot * n_row + row_at
        if slot < tail_first:
            start = tile_row * tile
        else:
            tail_start = n_columns * tile + (slot - tail_first) * tile
            start = jnp.where(tile_row < n_columns, tile_row * tile, tail_start)
        picked = lax.dynamic_slice_in_dim(factor, start, tile, axis=0)
        picked = picked.reshape(tile, col_slot_count, n_col, tile)
        picked = lax.dynamic_index_in_dim(picked, col_at, axis=2, keepdims=False)
        outs.append(picked)
    return jnp.stack(outs, axis=0)


def solution(mesh):
    in_specs = (P(None, "row", None, "col"), P(None, "row"), P(None, "col"))
    out_specs = P(None, "row", None, "col")
    return jax.shard_map(shards, mesh=mesh, in_specs=in_specs, out_specs=out_specs, check_vma=False)
```
